256 devices in a mesh: row: 8 (over z), col: 32 (over y, x, core).
Axes of the slice: x: 4, y: 4, z: 8, core: 2. Of those that a mesh axis runs over, the one named last changes fastest.
Arguments:
- front_matrix: bfloat16 [32768, 32768], P('row', 'col'), may hold values from -0.03125 to 0.03125
- right_random: bfloat16 [32768, 128], P(('col', 'row')), may hold values from -32 to 32
- left_random: bfloat16 [32768, 128], P(('row', 'col')), may hold values from -32 to 32
- row_basis: bfloat16 [32768, 384], P('row'), may hold values from -1 to 1, as said below
- column_basis: bfloat16 [32768, 384], P('col'), may hold values from -1 to 1, as said below
Outputs:
- row_samples: float32 [128, 32768], P('col', 'row')
- column_samples: float32 [128, 32768], P('row', 'col')
- row_spread: float32 [64], P('row')
- column_spread: float32 [64], P('col')
The draws below stay inside these ranges and needn't reach their ends.
Inputs may be any that keep to these rules, and one draw needn't show every extreme that they name: Within each leaf node's 512 rows, the columns of row_basis are orthonormal up to their rounding to bfloat16. Within each leaf node's 512 rows, the columns of column_basis are orthonormal up to their rounding to bfloat16.
All inputs are finite; a program needn't handle non-finite values.
Results may differ from the reference program's by a relative error of at most 0.0003.
Values may be sent and summed in bfloat16 or wider, within the bound.
A program may use at most 64 MiB of HBM per device.

```python
import jax
import jax.numpy as jnp
from jax import lax

N = 32768
SAMPLES = 128
EARLIER = 384
NODE = 512


def node_orthonormal(key):
    normals = jax.random.normal(key, (N // NODE, NODE, EARLIER), jnp.float32)
    factors, _ = jnp.linalg.qr(normals)
    return factors.reshape(N, EARLIER).astype(jnp.bfloat16)


def rising_block(key):
    position = jnp.arange(SAMPLES, dtype=jnp.float32) / (SAMPLES - 1)
    entries = jnp.clip(jax.random.normal(key, (N, SAMPLES), jnp.float32), -4.0, 4.0)
    scales = jnp.exp(position * jnp.log(4.0))
    return (entries * scales[None, :]).astype(jnp.bfloat16)


def draw_right_random(key, part):
    return rising_block(jax.random.fold_in(key, 41))


def draw_left_random(key, part):
    return rising_block(jax.random.fold_in(key, 53))


def draw_row_basis(key, part):
    return node_orthonormal(jax.random.fold_in(key, 11))


def draw_column_basis(key, part):
    return node_orthonormal(jax.random.fold_in(key, 29))


def block_scale(own_key, dims, cuts, smallest, high):
    def one(dim, blocks):
        draws = jax.random.uniform(jax.random.fold_in(jax.random.fold_in(own_key, 6), dim), (blocks,), jnp.float32, smallest / len(cuts), high / len(cuts))
        return jnp.repeat(jnp.exp(draws), dims[dim] // blocks).reshape((-1,) + (1,) * (len(dims) - dim - 1))

    loudness = one(*cuts[0])
    for cut in cuts[1:]:
        loudness = loudness * one(*cut)
    return loudness


def normal_values(key, dims, spread, reach, pieces=(), held_as=jnp.bfloat16):
    drawn = spread * jax.random.normal(key, dims, jnp.float32)
    if pieces:
        drawn = drawn * block_scale(key, dims, pieces, -0.22, 0.18)
    return jnp.clip(drawn, -reach, reach).astype(held_as)


def setup_inputs(seed: int = 0) -> dict:
    splits = jax.random.split(jax.random.key(seed), 6)
    front_matrix = normal_values(splits[0], (N, N), N ** -0.5, 0.03125, ((0, 8), (1, 32)))
    right_random = draw_right_random(jax.random.fold_in(splits[5], 71), 0)
    left_random = draw_left_random(jax.random.fold_in(splits[5], 71), 0)
    row_basis = draw_row_basis(jax.random.fold_in(splits[5], 71), 0)
    column_basis = draw_column_basis(jax.random.fold_in(splits[5], 71), 0)
    return {"front_matrix": front_matrix, "right_random": right_random, "left_random": left_random, "row_basis": row_basis, "column_basis": column_basis}


def project_out(full_samples, basis):
    count = full_samples.shape[0]
    nodes = basis.shape[0] // NODE
    shaped = full_samples.astype(jnp.float32).reshape(count, nodes, NODE)
    stacked = basis.astype(jnp.float32).reshape(nodes, NODE, EARLIER)
    coeffs = jnp.einsum('knr,nre->kne', shaped, stacked, precision=lax.Precision.HIGHEST)
    correction = jnp.einsum('kne,nre->knr', coeffs, stacked, precision=lax.Precision.HIGHEST)
    cleaned = shaped - correction
    squares = lax.optimization_barrier(jnp.sum(cleaned * cleaned, axis=(0, 2)))
    return (cleaned.reshape(count, nodes * NODE), jnp.sqrt(squares / (SAMPLES * NODE)))

def reference(front_matrix, right_random, left_random, row_basis, column_basis):
    row_full = jnp.dot(front_matrix.astype(jnp.float32), right_random.astype(jnp.float32), preferred_element_type=jnp.float32).T
    column_full = jnp.dot(left_random.T.astype(jnp.float32), front_matrix.astype(jnp.float32), preferred_element_type=jnp.float32)
    row_samples, row_spread = project_out(row_full, row_basis)
    column_samples, column_spread = project_out(column_full, column_basis)
    return (row_samples, column_samples, row_spread, column_spread)
```

```python
import functools

import jax
import jax.numpy as jnp
from jax import lax
from jax.experimental import pallas as pl
from jax.experimental.pallas import tpu as pltpu
from jax.sharding import PartitionSpec as P

F32 = jnp.float32
BF16 = jnp.bfloat16
MESH = pl.DeviceIdType.MESH
NODE = 512
EARLIER = 384
SAMPLES = 128
NZ = 8
ROWS = 4096
COLS = 1024
QS = 4


def three_parts(value):
    hi = value.astype(BF16).astype(F32)
    rest = value - hi
    mid = rest.astype(BF16).astype(F32)
    low = rest - mid
    return jnp.concatenate([hi, mid, low], axis=0).astype(BF16)


def joined(stacked, count):
    return stacked[:count] + stacked[count : 2 * count] + stacked[2 * count :]


def coeffs_of(value, basis):
    out = lax.dot_general(
        three_parts(value), basis, (((1,), (0,)), ((), ())), preferred_element_type=F32
    )
    return joined(out, value.shape[0])


def correction_of(coeffs, basis):
    out = lax.dot_general(
        three_parts(coeffs), basis, (((1,), (1,)), ((), ())), preferred_element_type=F32
    )
    return joined(out, coeffs.shape[0])


def kernel(
    a_hbm, r_hbm, l_hbm, rb_hbm, cb_hbm,
    row_out, col_out, rs_out, cs_out,
    a_v, rg, l_raw, lg, rb_v, cb_v, rowacc, cacc, cr, sx, srecv,
    ra_aug, ra_fin, rb_aug, rb_fin, vrow, vrow_all, vcol, vcol_all,
    in_sem, a_sem,
    r_ss, r_rs, la_ss, la_rs, lb_ss, lb_rs, lp_ss, lp_rs,
    d_ss, d_rs, sa_ss, sa_rs, sb_ss, sb_rs, c_ss, c_rs,
    vr_ss, vr_rs, vc_ss, vc_rs,
):
    z = lax.axis_index("row")
    c = lax.axis_index("col")
    core = lax.rem(c, 2)
    other = 1 - core
    x = lax.rem(lax.div(c, 2), 4)
    y = lax.div(c, 8)
    a0 = core * y + other * x
    b0 = core * x + other * y
    stride_a = 2 + 6 * core
    stride_b = 8 - 6 * core

    def za(step):
        return lax.rem(z + step + NZ, NZ)

    def at_a(step):
        return lax.rem(a0 + step + 4, 4)

    def at_b(step):
        return lax.rem(b0 + step + 4, 4)

    def dev_a(step):
        return (z, at_a(step) * stride_a + b0 * stride_b + core)

    def dev_b(step):
        return (z, a0 * stride_a + at_b(step) * stride_b + core)

    def dev_z(step):
        return (za(step), c)

    partner = (z, c + 1 - 2 * core)

    def remote(src, dst, ssem, rsem, device):
        return pltpu.make_async_remote_copy(
            src_ref=src, dst_ref=dst, send_sem=ssem, recv_sem=rsem,
            device_id=device, device_id_type=MESH,
        )

    sent = []

    def send(copy):
        copy.start()
        sent.append(copy)

    r_in = pltpu.make_async_copy(r_hbm, rg.at[z], in_sem.at[0])
    l_in = pltpu.make_async_copy(l_hbm, l_raw, in_sem.at[1])
    r_in.start()
    l_in.start()
    a_in = []
    for part in range(8):
        rows = pl.ds(part * NODE, NODE)
        copy = pltpu.make_async_copy(a_hbm.at[rows], a_v.at[rows], a_sem.at[part])
        copy.start()
        a_in.append(copy)
    rb_in = pltpu.make_async_copy(rb_hbm, rb_v, in_sem.at[2])
    cb_in = pltpu.make_async_copy(cb_hbm, cb_v, in_sem.at[3])
    cb_in.start()
    rb_in.start()

    barrier = pltpu.get_barrier_semaphore()
    peers = [dev_z(1), dev_z(-1), dev_a(1), dev_a(-1), dev_b(1), dev_b(-1), partner]
    for peer in peers:
        pl.semaphore_signal(barrier, inc=1, device_id=peer, device_id_type=MESH)
    l_in.wait()
    own_u = a0 * 4 + b0
    lg[core, own_u] = l_raw[...].T
    r_in.wait()
    pl.semaphore_wait(barrier, len(peers))

    def r_copy(side, step):
        d = 1 if side == 0 else -1
        block = za(-d * (step - 1))
        if step < 4:
            ref = rg.at[block]
        else:
            ref = rg.at[block, pl.ds(64 * side, 64)]
        return remote(ref, ref, r_ss.at[side, step - 1], r_rs.at[side, step - 1], dev_z(d))

    def r_forward(step):
        for side in (0, 1):
            r_copy(side, step).wait_recv()
            if step < 4:
                send(r_copy(side, step + 1))

    def l_slot(ra, rb):
        return at_a(ra) * 4 + at_b(rb)

    def la_full(side):
        d = 1 if side == 0 else -1
        ref = lg.at[core, own_u]
        return remote(ref, ref, la_ss.at[0, side], la_rs.at[0, side], dev_a(d))

    def la_half(side):
        d = 1 if side == 0 else -1
        ref = lg.at[core, l_slot(-d, 0), pl.ds(64 * side, 64)]
        return remote(ref, ref, la_ss.at[1, side], la_rs.at[1, side], dev_a(d))

    def lb_full(ra, side):
        d = 1 if side == 0 else -1
        ref = lg.at[core, l_slot(ra, 0)]
        return remote(ref, ref, lb_ss.at[0, ra, side], lb_rs.at[0, ra, side], dev_b(d))

    def lb_half(ra, side):
        d = 1 if side == 0 else -1
        ref = lg.at[core, l_slot(ra, -d), pl.ds(64 * side, 64)]
        return remote(ref, ref, lb_ss.at[1, ra, side], lb_rs.at[1, ra, side], dev_b(d))

    def lp(ra, rb):
        ref = lg.at[core, l_slot(ra, rb)]
        return remote(ref, ref, lp_ss.at[ra, rb], lp_rs.at[ra, rb], partner)

    def lb_arrived(ra):
        for side in (0, 1):
            lb_full(ra, side).wait_recv()
            send(lb_half(ra, side))
        for side in (0, 1):
            send(lp(ra, 3 if side == 0 else 1))

    def lb_two_arrived(ra):
        for side in (0, 1):
            lb_half(ra, side).wait_recv()
        send(lp(ra, 2))

    def row_term(rows, one, two, weights):
        left = jnp.concatenate(
            [
                a_v[rows, pl.ds(pl.multiple_of(one * 128, 128), 128)],
                a_v[rows, pl.ds(pl.multiple_of(two * 128, 128), 128)],
            ],
            axis=1,
        )
        return jnp.dot(left, weights, preferred_element_type=F32)

    def r_pair(one, two):
        return jnp.concatenate([rg[one], rg[two]], axis=0)

    def row_pass(one, two, first):
        weights = r_pair(one, two)

        def body(part, carry):
            rows = pl.ds(pl.multiple_of(part * NODE, NODE), NODE)
            term = row_term(rows, one, two, weights)
            if first:
                rowacc[rows, :] = term
            else:
                rowacc[rows, :] += term
            return carry

        lax.fori_loop(0, 8, body, 0)

    def col_pass(mine, rb, first):
        if mine:
            cc, sa, sb, b_at = core, stride_a, stride_b, at_b(rb)
        else:
            cc, sa, sb = other, 2 + 6 * other, 8 - 6 * other
            b_at = lax.rem(a0 + rb, 4)
        left = jnp.concatenate([lg[cc, a * 4 + b_at] for a in range(4)], axis=1)
        starts = [pl.multiple_of((a * sa + b_at * sb + cc) * 128, 128) for a in range(4)]

        def body(part, carry):
            lanes = pl.ds(pl.multiple_of(part * 256, 256), 256)
            right = jnp.concatenate([a_v[pl.ds(s, 128), lanes] for s in starts], axis=0)
            term = jnp.dot(left, right, preferred_element_type=F32).reshape(NZ, 2, 8, 256)
            if first:
                cacc[:, :, :, lanes] = term
            else:
                cacc[:, :, :, lanes] += term
            return carry

        lax.fori_loop(0, 4, body, 0)

    for side in (0, 1):
        send(r_copy(side, 1))
    for side in (0, 1):
        send(la_full(side))
        send(lb_full(0, side))
    send(lp(0, 0))

    r_forward(1)
    for side in (0, 1):
        la_full(side).wait_recv()
        send(la_half(side))
        ra = 3 if side == 0 else 1
        send(lb_full(ra, 0))
        send(lb_full(ra, 1))
    send(lp(3, 0))
    send(lp(1, 0))
    lb_arrived(0)
    for copy in a_in:
        copy.wait()
    row_pass(za(1), za(-1), True)

    r_forward(2)
    for side in (0, 1):
        la_half(side).wait_recv()
    send(lb_full(2, 0))
    send(lb_full(2, 1))
    send(lp(2, 0))
    lb_arrived(1)
    lb_arrived(3)
    lb_two_arrived(0)
    row_pass(za(2), za(-2), False)
    col_pass(True, 0, True)

    r_forward(3)
    lb_arrived(2)
    lb_two_arrived(1)
    lb_two_arrived(3)
    row_pass(za(3), za(-3), False)
    col_pass(True, 1, False)
    col_pass(True, 3, False)
    for ra in range(4):
        lp(ra, 0).wait_recv()
    col_pass(False, 0, False)

    lb_two_arrived(2)
    r_forward(4)

    weights = r_pair(z, za(4))
    sub = lax.broadcasted_iota(jnp.int32, (16, 8, NODE), 1)

    def d_copy(q):
        return remote(sx.at[other, q], srecv.at[q], d_ss.at[q], d_rs.at[q], partner)

    for q in range(QS):
        halves = []
        for h in (0, 1):
            rows = pl.ds((q + 4 * h) * NODE, NODE)
            total = rowacc[rows, :] + row_term(rows, z, za(4), weights)
            halves.append(total.T.reshape(16, 8, NODE))
        low, high = halves
        to0 = jnp.where(sub < 4, low, pltpu.roll(high, 4, 1))
        to1 = jnp.where(sub < 4, pltpu.roll(low, 4, 1), high)
        for t in range(16):
            ty, tx = t // 4, t % 4
            sx[0, q, tx * 4 + ty] = to0[t]
            sx[1, q, ty * 4 + tx] = to1[t]
        send(d_copy(q))

    for rb in (1, 3):
        for ra in range(4):
            lp(ra, rb).wait_recv()
        col_pass(False, rb, False)
    col_pass(True, 2, False)
    for ra in range(4):
        lp(ra, 2).wait_recv()
    col_pass(False, 2, False)

    def hops(side, h):
        return 4 if side == h else 3

    def c_copy(side, reach, h, n):
        d = 1 if side == 0 else -1
        return remote(
            cacc.at[za(d * reach), h, :, pl.ds(n * NODE, NODE)],
            cr.at[side, reach - 1, h, n],
            c_ss.at[side, reach - 1, h, n],
            c_rs.at[side, reach - 1, h, n],
            dev_z(d),
        )

    def c_step(step):
        for h_first in (True, False):
            for n in (0, 1):
                for side in (0, 1):
                    h = side if h_first else 1 - side
                    reach = hops(side, h) - step + 1
                    if reach < 2:
                        continue
                    d = 1 if side == 0 else -1
                    c_copy(side, reach, h, n).wait_recv()
                    lanes = pl.ds(n * NODE, NODE)
                    cacc[za(d * (reach - 1)), h, :, lanes] += cr[side, reach - 1, h, n]
                    send(c_copy(side, reach - 1, h, n))

    for h_first in (True, False):
        for n in (0, 1):
            for side in (0, 1):
                h = side if h_first else 1 - side
                send(c_copy(side, hops(side, h), h, n))

    def sa_copy(kind, q, side):
        d = 1 if side == 0 else -1
        if kind == 0:
            src = sx.at[core, q, pl.ds(at_a(2) * 4 + 2 * side, 2)]
            dst = ra_aug.at[side, q]
        else:
            half = 1 - side if kind == 1 else side
            src = sx.at[core, q, pl.ds(at_a(d) * 4 + 2 * half, 2)]
            dst = ra_fin.at[side, q, half]
        return remote(src, dst, sa_ss.at[kind, q, side], sa_rs.at[kind, q, side], dev_a(d))

    def sb_copy(kind, q, side):
        d = 1 if side == 0 else -1
        if kind == 0:
            src = sx.at[core, q, a0 * 4 + at_b(2), :, pl.ds(256 * side, 256)]
            dst = rb_aug.at[side, q]
        else:
            half = 1 - side if kind == 1 else side
            src = sx.at[core, q, a0 * 4 + at_b(d), :, pl.ds(256 * half, 256)]
            dst = rb_fin.at[side, q, half]
        return remote(src, dst, sb_ss.at[kind, q, side], sb_rs.at[kind, q, side], dev_b(d))

    for q in range(QS):
        d_copy(q).wait_recv()
        sx[core, q] += srecv[q]
        for kind in (0, 1):
            for side in (0, 1):
                send(sa_copy(kind, q, side))
    c_step(1)
    for q in range(QS):
        for side in (0, 1):
            d = 1 if side == 0 else -1
            sa_copy(0, q, side).wait_recv()
            sx[core, q, pl.ds(at_a(d) * 4 + 2 * side, 2)] += ra_aug[side, q]
            send(sa_copy(2, q, side))
    c_step(2)
    for q in range(QS):
        for kind in (1, 2):
            for side in (0, 1):
                sa_copy(kind, q, side).wait_recv()
        for half in (0, 1):
            sx[core, q, pl.ds(a0 * 4 + 2 * half, 2)] += ra_fin[0, q, half] + ra_fin[1, q, half]
        for kind in (0, 1):
            for side in (0, 1):
                send(sb_copy(kind, q, side))
    c_step(3)
    for q in range(QS):
        for side in (0, 1):
            d = 1 if side == 0 else -1
            sb_copy(0, q, side).wait_recv()
            sx[core, q, a0 * 4 + at_b(d), :, pl.ds(256 * side, 256)] += rb_aug[side, q]
            send(sb_copy(2, q, side))

    lane8 = lax.broadcasted_iota(jnp.int32, (8, 128), 1)
    sub8 = lax.broadcasted_iota(jnp.int32, (8, 128), 0)
    cb_in.wait()
    col_sq = jnp.zeros((8, 128), F32)
    for n in (0, 1):
        lanes = pl.ds(n * NODE, NODE)
        parts = []
        for h in (0, 1):
            for side in (0, 1):
                c_copy(side, 1, h, n).wait_recv()
            parts.append(cacc[z, h, :, lanes] + cr[0, 0, h, n] + cr[1, 0, h, n])
        full = jnp.concatenate(parts, axis=0)
        basis = cb_v[pl.ds(n * NODE, NODE), :]
        cleaned = full - correction_of(coeffs_of(full, basis), basis)
        col_out[:, lanes] = cleaned
        sq = jnp.sum(cleaned * cleaned, axis=1, keepdims=True)
        col_sq = col_sq + jnp.where(lane8 == n, sq[:8] + sq[8:], 0.0)
    vcol[...] = col_sq

    def vc_copy(j):
        return remote(vcol, vcol_all.at[j], vc_ss.at[j], vc_rs.at[j], dev_z(j))

    def vr_copy(j):
        return remote(
            vrow, vrow_all.at[j], vr_ss.at[j], vr_rs.at[j], (z, lax.rem(c + j, 32))
        )

    def loop(first, last, what):
        def body(j, carry):
            what(j)
            return carry

        lax.fori_loop(first, last, body, 0)

    loop(1, NZ, lambda j: vc_copy(j).start())

    rb_in.wait()
    row_sq = jnp.zeros((8, 128), F32)
    sub_n = lax.broadcasted_iota(jnp.int32, (8, EARLIER), 0)
    sub_r = lax.broadcasted_iota(jnp.int32, (8, NODE), 0)
    for q in range(QS):
        for kind in (1, 2):
            for side in (0, 1):
                sb_copy(kind, q, side).wait_recv()
        full = sx[core, q, own_u] + jnp.concatenate(
            [rb_fin[0, q, h] + rb_fin[1, q, h] for h in (0, 1)], axis=1
        )
        low_basis = rb_v[pl.ds(q * NODE, NODE), :]
        high_basis = rb_v[pl.ds((q + 4) * NODE, NODE), :]
        coeffs = jnp.where(
            sub_n < 4, coeffs_of(full, low_basis), coeffs_of(full, high_basis)
        )
        correction = jnp.where(
            sub_r < 4, correction_of(coeffs, low_basis), correction_of(coeffs, high_basis)
        )
        cleaned = full - correction
        row_out[:, pl.ds(q * NODE, NODE)] = cleaned[:4]
        row_out[:, pl.ds((q + 4) * NODE, NODE)] = cleaned[4:]
        sq = jnp.sum(cleaned * cleaned, axis=1, keepdims=True)
        place = jnp.where(sub8 < 4, q, q + 4)
        row_sq = row_sq + jnp.where(lane8 == place, sq, 0.0)
    vrow[...] = row_sq
    loop(1, 32, lambda j: vr_copy(j).start())

    loop(1, NZ, lambda j: vc_copy(j).wait_recv())
    col_total = vcol[...]
    for j in range(1, NZ):
        col_total = col_total + vcol_all[j]
    scale = 1.0 / (SAMPLES * NODE)
    col_lane = jnp.sum(col_total, axis=0, keepdims=True)
    cs_out[...] = jnp.sqrt(col_lane * scale)[:, :2]

    for copy in sent:
        copy.wait_send()
    loop(1, NZ, lambda j: vc_copy(j).wait_send())

    loop(1, 32, lambda j: vr_copy(j).wait_recv())
    row_total = vrow[...]
    for j in range(1, 32):
        row_total = row_total + vrow_all[j]
    row_lane = jnp.sum(row_total, axis=0, keepdims=True)
    rs_out[...] = jnp.sqrt(row_lane * scale)[:, :8]
    loop(1, 32, lambda j: vr_copy(j).wait_send())


def shards(front_matrix, right_random, left_random, row_basis, column_basis):
    vmem = pltpu.VMEM
    dma = pltpu.SemaphoreType.DMA
    row, col, rs, cs = pl.pallas_call(
        kernel,
        out_shape=(
            jax.ShapeDtypeStruct((4, ROWS), F32),
            jax.ShapeDtypeStruct((16, COLS), F32),
            jax.ShapeDtypeStruct((1, 8), F32),
            jax.ShapeDtypeStruct((1, 2), F32),
        ),
        in_specs=[pl.BlockSpec(memory_space=pl.ANY)] * 5,
        out_specs=[pl.BlockSpec(memory_space=pltpu.VMEM)] * 4,
        scratch_shapes=[
            vmem((ROWS, COLS), BF16),
            vmem((NZ, 128, 128), BF16),
            vmem((128, 128), BF16),
            vmem((2, 16, 128, 128), BF16),
            vmem((ROWS, EARLIER), BF16),
            vmem((COLS, EARLIER), BF16),
            vmem((ROWS, 128), F32),
            vmem((NZ, 2, 8, COLS), F32),
            vmem((2, 4, 2, 2, 8, NODE), F32),
            vmem((2, QS, 16, 8, NODE), F32),
            vmem((QS, 16, 8, NODE), F32),
            vmem((2, QS, 2, 8, NODE), F32),
            vmem((2, QS, 2, 2, 8, NODE), F32),
            vmem((2, QS, 8, 256), F32),
            vmem((2, QS, 2, 8, 256), F32),
            vmem((8, 128), F32),
            vmem((32, 8, 128), F32),
            vmem((8, 128), F32),
            vmem((NZ, 8, 128), F32),
            dma((4,)), dma((8,)),
            dma((2, 4)), dma((2, 4)),
            dma((2, 2)), dma((2, 2)),
            dma((2, 4, 2)), dma((2, 4, 2)),
            dma((4, 4)), dma((4, 4)),
            dma((QS,)), dma((QS,)),
            dma((3, QS, 2)), dma((3, QS, 2)),
            dma((3, QS, 2)), dma((3, QS, 2)),
            dma((2, 4, 2, 2)), dma((2, 4, 2, 2)),
            dma((32,)), dma((32,)),
            dma((NZ,)), dma((NZ,)),
        ],
        compiler_params=pltpu.CompilerParams(
            collective_id=0, has_side_effects=True, vmem_limit_bytes=48 * 1024 * 1024
        ),
        name="hss_sample",
    )(front_matrix, right_random, left_random, row_basis, column_basis)
    return row, col, rs.reshape(8), cs.reshape(2)


def solution(mesh):
    return jax.shard_map(
        shards,
        mesh=mesh,
        in_specs=(
            P("row", "col"), P(("col", "row"), None), P(("row", "col"), None),
            P("row", None), P("col", None),
        ),
        out_specs=(P("col", "row"), P("row", "col"), P("row"), P("col")),
        check_vma=False,
    )
```

```python
import functools

import jax
import jax.numpy as jnp
from jax import lax
from jax.experimental import pallas as pl
from jax.experimental.pallas import tpu as pltpu
from jax.sharding import PartitionSpec as P

F32 = jnp.float32
BF16 = jnp.bfloat16
MESH = pl.DeviceIdType.MESH
NODE = 512
EARLIER = 384
SAMPLES = 128
NZ = 8
ROWS = 4096
COLS = 1024
QS = 4
VMEM_LIMIT = 67043328


def three_parts(value):
    hi = value.astype(BF16).astype(F32)
    rest = value - hi
    mid = rest.astype(BF16).astype(F32)
    low = rest - mid
    return jnp.concatenate([hi, mid, low], axis=0).astype(BF16)


def joined(stacked, count):
    return stacked[:count] + stacked[count : 2 * count] + stacked[2 * count :]


def parts_dot(value, other, contract):
    out = lax.dot_general(
        three_parts(value), other, (((1,), (contract,)), ((), ())), preferred_element_type=F32
    )
    return joined(out, value.shape[0])


def kernel(
    a_hbm, r_hbm, l_hbm, rb_hbm, cb_hbm,
    row_hbm, col_hbm, rs_hbm, cs_hbm,
    row_out, col_out, rs_out, cs_out,
    a_v, rg, r_raw, l_raw, lg, rb_v, rbt, cb_v, rowacc, cacc, cr, cr4, sx, srecv, tb,
    ra_aug, ra_fin, rb_fin, vrow, vrow_all, vcol, vcol_all,
    in_sem, out_sem, a_sem,
    r_ss, r_rs, la_ss, la_rs, lb_ss, lb_rs, lp_ss, lp_rs,
    d_ss, d_rs, sa_ss, sa_rs, sb_ss, sb_rs, c_ss, c_rs,
    vr_ss, vr_rs, vc_ss, vc_rs,
):
    z = lax.axis_index("row")
    c = lax.axis_index("col")
    core = lax.rem(c, 2)
    other = 1 - core
    x = lax.rem(lax.div(c, 2), 4)
    y = lax.div(c, 8)
    a0 = core * y + other * x
    b0 = core * x + other * y
    stride_a = 2 + 6 * core
    stride_b = 8 - 6 * core

    def za(step):
        return lax.rem(z + step + NZ, NZ)

    def at_a(step):
        return lax.rem(a0 + step + 4, 4)

    def at_b(step):
        return lax.rem(b0 + step + 4, 4)

    def dev_a(step):
        return (z, at_a(step) * stride_a + b0 * stride_b + core)

    def dev_b(step):
        return (z, a0 * stride_a + at_b(step) * stride_b + core)

    def dev_z(step):
        return (za(step), c)

    partner = (z, c + 1 - 2 * core)

    def remote(src, dst, ssem, rsem, device):
        return pltpu.make_async_remote_copy(
            src_ref=src, dst_ref=dst, send_sem=ssem, recv_sem=rsem,
            device_id=device, device_id_type=MESH,
        )

    sent = []

    def send(copy):
        copy.start()
        sent.append(copy)

    r_in = pltpu.make_async_copy(r_hbm, r_raw, in_sem.at[0])
    l_in = pltpu.make_async_copy(l_hbm, l_raw, in_sem.at[1])
    r_in.start()
    l_in.start()
    barrier = pltpu.get_barrier_semaphore()
    peers = [dev_z(1), dev_z(-1), dev_a(1), dev_a(-1), dev_b(1), dev_b(-1), partner]
    for peer in peers:
        pl.semaphore_signal(barrier, inc=1, device_id=peer, device_id_type=MESH)
    l_in.wait()
    own_u = a0 * 4 + b0
    lg[core, own_u] = l_raw[...].T
    r_in.wait()
    rg[z] = r_raw[...].T
    rb_in = pltpu.make_async_copy(rb_hbm, rb_v, in_sem.at[2])
    cb_in = pltpu.make_async_copy(cb_hbm, cb_v, in_sem.at[3])
    rb_in.start()
    a_in = []
    for part in range(8):
        rows = pl.ds(part * NODE, NODE)
        copy = pltpu.make_async_copy(a_hbm.at[rows], a_v.at[rows], a_sem.at[part])
        copy.start()
        a_in.append(copy)
    cb_in.start()
    pl.semaphore_wait(barrier, len(peers))

    def r_copy(side, kind):
        d = 1 if side == 0 else -1
        block = za((0, -d, -d, -3 * d)[kind])
        reach = (d, d, 2 * d, d)[kind]
        ref = rg.at[block] if kind < 3 else rg.at[block, pl.ds(64 * side, 64)]
        return remote(ref, ref, r_ss.at[side, kind], r_rs.at[side, kind], dev_z(reach))

    def l_slot(ra, rb):
        return at_a(ra) * 4 + at_b(rb)

    def la_full(side):
        d = 1 if side == 0 else -1
        ref = lg.at[core, own_u]
        return remote(ref, ref, la_ss.at[0, side], la_rs.at[0, side], dev_a(d))

    def la_half(side):
        d = 1 if side == 0 else -1
        ref = lg.at[core, l_slot(-d, 0), pl.ds(64 * side, 64)]
        return remote(ref, ref, la_ss.at[1, side], la_rs.at[1, side], dev_a(d))

    def lb_full(ra, side):
        d = 1 if side == 0 else -1
        ref = lg.at[core, l_slot(ra, 0)]
        return remote(ref, ref, lb_ss.at[0, ra, side], lb_rs.at[0, ra, side], dev_b(d))

    def lb_two(ra):
        ref = lg.at[core, l_slot(ra, 0)]
        return remote(ref, ref, lb_ss.at[1, ra, 0], lb_rs.at[1, ra, 0], dev_b(2))

    def lp(ra, rb):
        ref = lg.at[core, l_slot(ra, rb)]
        return remote(ref, ref, lp_ss.at[ra, rb], lp_rs.at[ra, rb], partner)

    def lb_arrived(ra):
        for side in (0, 1):
            lb_full(ra, side).wait_recv()
            send(lp(ra, 3 if side == 0 else 1))

    def lb_two_arrived(ra):
        lb_two(ra).wait_recv()
        send(lp(ra, 2))

    def row_term(node, blocks, left):
        rows = pl.ds(pl.multiple_of(node * NODE, NODE), NODE)
        right = jnp.concatenate(
            [a_v[rows, pl.ds(pl.multiple_of(k * 128, 128), 128)] for k in blocks], axis=1
        )
        return lax.dot_general(
            left, right, (((1,), (1,)), ((), ())), preferred_element_type=F32
        )

    def row_pass(blocks):
        left = jnp.concatenate([rg[k] for k in blocks], axis=1)

        def body(part, carry):
            for node in (2 * part, 2 * part + 1):
                rowacc[node] = row_term(node, blocks, left)
            return carry

        lax.fori_loop(0, 4, body, 0)

    def col_pass(groups, first):
        lefts, starts = [], []
        for mine, ra in groups:
            if mine:
                cc, sa, sb, a_at = core, stride_a, stride_b, at_a(ra)
            else:
                cc, sa, sb = other, 2 + 6 * other, 8 - 6 * other
                a_at = lax.rem(b0 + ra, 4)
            for b in range(4):
                lefts.append(lg[cc, a_at * 4 + b])
                starts.append(pl.multiple_of((a_at * sa + b * sb + cc) * 128, 128))
        left = jnp.concatenate(lefts, axis=1)
        right = jnp.concatenate([a_v[pl.ds(s, 128), :] for s in starts], axis=0)
        term = jnp.dot(left, right, preferred_element_type=F32).reshape(NZ, 2, 8, COLS)
        if first:
            cacc[...] = term
        else:
            cacc[...] += term

    for side in (0, 1):
        send(r_copy(side, 0))
    for side in (0, 1):
        send(la_full(side))
        send(lb_full(0, side))
    send(lp(0, 0))

    for side in (0, 1):
        r_copy(side, 0).wait_recv()
        send(r_copy(side, 1))
    for side in (0, 1):
        send(r_copy(side, 2))
    for side in (0, 1):
        la_full(side).wait_recv()
        send(la_half(side))
        ra = 3 if side == 0 else 1
        send(lb_full(ra, 0))
        send(lb_full(ra, 1))
    lb_arrived(0)
    for ra in (1, 3, 0):
        send(lb_two(ra))
    send(lp(3, 0))
    send(lp(1, 0))
    rb_in.wait()

    def turn(n, carry):
        rows = pl.ds(pl.multiple_of(n * NODE, NODE), NODE)
        rbt[n] = rb_v[rows, :].T
        return carry

    lax.fori_loop(0, 8, turn, 0)

    for side in (0, 1):
        la_half(side).wait_recv()
    send(lb_full(2, 0))
    send(lb_full(2, 1))
    send(lb_two(2))
    send(lp(2, 0))
    for side in (0, 1):
        r_copy(side, 1).wait_recv()
        r_copy(side, 2).wait_recv()
        send(r_copy(side, 3))
    lb_arrived(1)
    lb_arrived(3)
    for ra in (0, 1, 3):
        lb_two_arrived(ra)
    for copy in a_in:
        copy.wait()
    row_pass([za(k) for k in (1, -1, 2, -2, 3, -3)])
    col_pass([(True, 0), (True, 1), (True, 3)], True)

    lb_arrived(2)
    lb_two_arrived(2)
    for side in (0, 1):
        r_copy(side, 3).wait_recv()

    last = [z, za(4)]
    left = jnp.concatenate([rg[k] for k in last], axis=1)
    sub = lax.broadcasted_iota(jnp.int32, (8, NODE), 0)

    def d_copy(q):
        return remote(sx.at[other, q], srecv.at[q], d_ss.at[q], d_rs.at[q], partner)

    for q in range(QS):
        for nn in (0, 1):
            total = rowacc[2 * q + nn] + row_term(2 * q + nn, last, left)
            v = total.reshape(16, 8, NODE)
            w = pltpu.roll(v, 4, 1)
            for one in range(4):
                for bp in (0, 1):
                    t0, t1 = 8 * bp + one, 8 * bp + 4 + one
                    sx[0, q, nn, one, bp] = jnp.where(sub < 4, v[t0], w[t1])
                    t0 = 4 * one + 2 * bp
                    sx[1, q, nn, one, bp] = jnp.where(sub < 4, w[t0], v[t0 + 1])
        send(d_copy(q))

    def c_copy(side, kind, n):
        d = 1 if side == 0 else -1
        lanes = pl.ds(n * NODE, NODE)
        if kind == 0:
            src, dst = cacc.at[za(4), side, :, lanes], cr4.at[side, n]
        else:
            src = cacc.at[za((0, 3 * d, d, 2 * d)[kind]), :, :, lanes]
            dst = cr.at[kind - 1, side, n]
        reach = (2 * d, d, d, 2 * d)[kind]
        return remote(
            src, dst, c_ss.at[kind, side, n], c_rs.at[kind, side, n], dev_z(reach)
        )

    def sa_copy(kind, q, side):
        d = 1 if side == 0 else -1
        if kind == 0:
            src = sx.at[core, q, side, at_a(2)]
            dst = ra_aug.at[side, q]
        else:
            half = 1 - side if kind == 1 else side
            src = sx.at[core, q, half, at_a(d)]
            dst = ra_fin.at[side, q, half]
        return remote(src, dst, sa_ss.at[kind, q, side], sa_rs.at[kind, q, side], dev_a(d))

    def sb_copy(q, step):
        return remote(
            tb.at[q, at_b(step)], rb_fin.at[step, q],
            sb_ss.at[step, q], sb_rs.at[step, q], dev_b(step),
        )

    def chip_sum(q):
        d_copy(q).wait_recv()
        full = [(sx[core, q, nn] + srecv[q, nn]).reshape(64, NODE) for nn in (0, 1)]
        coeffs = [
            parts_dot(full[nn], rb_v[pl.ds((2 * q + nn) * NODE, NODE), :], 0) for nn in (0, 1)
        ]
        cleaned = [full[nn] - parts_dot(coeffs[nn], rbt[2 * q + nn], 0) for nn in (0, 1)]
        for nn in (0, 1):
            sx[core, q, nn] = cleaned[nn].reshape(4, 2, 8, NODE)
        for kind in (0, 1):
            for side in (0, 1):
                send(sa_copy(kind, q, side))

    def a_added(q):
        for side in (0, 1):
            d = 1 if side == 0 else -1
            sa_copy(0, q, side).wait_recv()
            sx[core, q, side, at_a(d)] += ra_aug[side, q]
            send(sa_copy(2, q, side))

    def a_summed(q):
        for kind in (1, 2):
            for side in (0, 1):
                sa_copy(kind, q, side).wait_recv()
        low = sx[core, q, 0, a0] + ra_fin[0, q, 0] + ra_fin[1, q, 0]
        high = sx[core, q, 1, a0] + ra_fin[0, q, 1] + ra_fin[1, q, 1]
        low_rolled, high_rolled = pltpu.roll(low, 4, 1), pltpu.roll(high, 4, 1)
        for bp in (0, 1):
            tb[q, 2 * bp] = jnp.where(sub < 4, low[bp], high_rolled[bp])
            tb[q, 2 * bp + 1] = jnp.where(sub < 4, low_rolled[bp], high[bp])
        for step in (1, 3, 2):
            send(sb_copy(q, step))

    for ra in range(4):
        for rb in range(4):
            lp(ra, rb).wait_recv()
    col_pass([(True, 2), (False, 0), (False, 1), (False, 3), (False, 2)], False)

    for n in (0, 1):
        for kind in (0, 1):
            for side in (0, 1):
                send(c_copy(side, kind, n))
    for n in (0, 1):
        for side in (0, 1):
            send(c_copy(side, 2, n))

    def c_added(n):
        lanes = pl.ds(n * NODE, NODE)
        for side in (0, 1):
            two = za(2 if side == 0 else -2)
            c_copy(side, 0, n).wait_recv()
            c_copy(side, 1, n).wait_recv()
            cacc[two, :, :, lanes] += cr[0, side, n]
            cacc[two, side, :, lanes] += cr4[side, n]
            send(c_copy(side, 3, n))

    chip_sum(0)
    chip_sum(1)
    chip_sum(2)
    chip_sum(3)
    a_added(0)
    c_added(0)
    a_added(1)
    c_added(1)
    a_added(2)
    a_added(3)
    a_summed(0)
    a_summed(1)
    a_summed(2)
    a_summed(3)

    lane8 = lax.broadcasted_iota(jnp.int32, (8, 128), 1)
    sub8 = lax.broadcasted_iota(jnp.int32, (8, 128), 0)
    cb_in.wait()
    col_sq = jnp.zeros((8, 128), F32)
    for n in (0, 1):
        lanes = pl.ds(n * NODE, NODE)
        for side in (0, 1):
            for kind in (2, 3):
                c_copy(side, kind, n).wait_recv()
        full = cacc[z, :, :, lanes] + cr[1, 0, n] + cr[1, 1, n] + cr[2, 0, n] + cr[2, 1, n]
        full = full.reshape(16, NODE)
        basis = cb_v[pl.ds(n * NODE, NODE), :]
        cleaned = full - parts_dot(parts_dot(full, basis, 0), basis, 1)
        col_out[:, lanes] = cleaned
        sq = jnp.sum(cleaned * cleaned, axis=1, keepdims=True)
        col_sq = col_sq + jnp.where(lane8 == n, sq[:8] + sq[8:], 0.0)
    vcol[...] = jnp.sum(col_sq, axis=0, keepdims=True)
    stores = [
        pltpu.make_async_copy(src, dst, out_sem.at[k])
        for k, (src, dst) in enumerate(
            [(row_out, row_hbm), (col_out, col_hbm), (rs_out, rs_hbm), (cs_out, cs_hbm)]
        )
    ]

    def vc_copy(j):
        return remote(vcol, vcol_all.at[j], vc_ss.at[j], vc_rs.at[j], dev_z(j))

    def vr_copy(j):
        return remote(
            vrow, vrow_all.at[j], vr_ss.at[j], vr_rs.at[j], (z, lax.rem(c + j, 32))
        )

    def loop(first, last, what):
        def body(j, carry):
            what(j)
            return carry

        lax.fori_loop(first, last, body, 0)

    loop(1, NZ, lambda j: vc_copy(j).start())
    stores[1].start()

    row_sq = jnp.zeros((8, 128), F32)
    for q in range(QS):
        for step in (1, 3, 2):
            sb_copy(q, step).wait_recv()
        cleaned = tb[q, b0] + rb_fin[1, q] + rb_fin[3, q] + rb_fin[2, q]
        row_out[:, pl.ds(2 * q * NODE, NODE)] = cleaned[:4]
        row_out[:, pl.ds((2 * q + 1) * NODE, NODE)] = cleaned[4:]
        sq = jnp.sum(cleaned * cleaned, axis=1, keepdims=True)
        place = jnp.where(sub8 < 4, 2 * q, 2 * q + 1)
        row_sq = row_sq + jnp.where(lane8 == place, sq, 0.0)
    vrow[...] = jnp.sum(row_sq, axis=0, keepdims=True)
    loop(1, 32, lambda j: vr_copy(j).start())
    stores[0].start()

    loop(1, NZ, lambda j: vc_copy(j).wait_recv())
    col_total = vcol[...]
    for j in range(1, NZ):
        col_total = col_total + vcol_all[j]
    scale = 1.0 / (SAMPLES * NODE)
    cs_out[...] = jnp.sqrt(col_total * scale)[:, :2]
    stores[3].start()

    for copy in sent:
        copy.wait_send()
    loop(1, NZ, lambda j: vc_copy(j).wait_send())

    loop(1, 32, lambda j: vr_copy(j).wait_recv())
    row_total = vrow[...]
    for j in range(1, 32):
        row_total = row_total + vrow_all[j]
    rs_out[...] = jnp.sqrt(row_total * scale)[:, :8]
    stores[2].start()
    loop(1, 32, lambda j: vr_copy(j).wait_send())
    for copy in stores:
        copy.wait()


def store_kernel(*refs):
    given, stored, held, sem = refs[:4], refs[4:8], refs[8:12], refs[12]
    loads = [pltpu.make_async_copy(given[k], held[k], sem.at[0, k]) for k in range(4)]
    stores = [pltpu.make_async_copy(held[k], stored[k], sem.at[1, k]) for k in range(4)]
    for copy in loads:
        copy.start()
    for load, store in zip(loads, stores):
        load.wait()
        store.start()
    for copy in stores:
        copy.wait()


def shards(front_matrix, right_random, left_random, row_basis, column_basis):
    vmem = pltpu.VMEM
    dma = pltpu.SemaphoreType.DMA
    row, col, rs, cs = pl.pallas_call(
        kernel,
        out_shape=(
            jax.ShapeDtypeStruct((4, ROWS), F32),
            jax.ShapeDtypeStruct((16, COLS), F32),
            jax.ShapeDtypeStruct((1, 8), F32),
            jax.ShapeDtypeStruct((1, 2), F32),
        ),
        in_specs=[pl.BlockSpec(memory_space=pltpu.HBM)] * 5,
        out_specs=[pl.BlockSpec(memory_space=pltpu.HBM)] * 4,
        scratch_shapes=[
            vmem((4, ROWS), F32), vmem((16, COLS), F32), vmem((1, 8), F32), vmem((1, 2), F32),
            vmem((ROWS, COLS), BF16),
            vmem((NZ, 128, 128), BF16),
            vmem((128, 128), BF16),
            vmem((128, 128), BF16),
            vmem((2, 16, 128, 128), BF16),
            vmem((ROWS, EARLIER), BF16),
            vmem((8, EARLIER, NODE), BF16),
            vmem((COLS, EARLIER), BF16),
            vmem((8, 128, NODE), F32),
            vmem((NZ, 2, 8, COLS), F32),
            vmem((3, 2, 2, 2, 8, NODE), F32),
            vmem((2, 2, 8, NODE), F32),
            vmem((2, QS, 2, 4, 2, 8, NODE), F32),
            vmem((QS, 2, 4, 2, 8, NODE), F32),
            vmem((QS, 4, 8, NODE), F32),
            vmem((2, QS, 2, 8, NODE), F32),
            vmem((2, QS, 2, 2, 8, NODE), F32),
            vmem((4, QS, 8, NODE), F32),
            vmem((1, 128), F32),
            vmem((32, 1, 128), F32),
            vmem((1, 128), F32),
            vmem((NZ, 1, 128), F32),
            dma((4,)), dma((4,)), dma((8,)),
            dma((2, 4)), dma((2, 4)),
            dma((2, 2)), dma((2, 2)),
            dma((2, 4, 2)), dma((2, 4, 2)),
            dma((4, 4)), dma((4, 4)),
            dma((QS,)), dma((QS,)),
            dma((3, QS, 2)), dma((3, QS, 2)),
            dma((4, QS)), dma((4, QS)),
            dma((4, 2, 2)), dma((4, 2, 2)),
            dma((32,)), dma((32,)),
            dma((NZ,)), dma((NZ,)),
        ],
        compiler_params=pltpu.CompilerParams(
            collective_id=0, has_side_effects=True, vmem_limit_bytes=VMEM_LIMIT
        ),
        name="hss_sample",
    )(front_matrix, right_random, left_random, row_basis, column_basis)
    results = (row, col, rs, cs)
    row, col, rs, cs = pl.pallas_call(
        store_kernel,
        out_shape=tuple(jax.ShapeDtypeStruct(v.shape, F32) for v in results),
        in_specs=[pl.BlockSpec(memory_space=pltpu.HBM)] * 4,
        out_specs=[pl.BlockSpec(memory_space=pltpu.HBM)] * 4,
        scratch_shapes=[vmem(v.shape, F32) for v in results] + [dma((2, 4))],
        compiler_params=pltpu.CompilerParams(vmem_limit_bytes=VMEM_LIMIT),
        name="store_results",
    )(*results)
    return row, col, rs.reshape(8), cs.reshape(2)


def solution(mesh):
    return jax.shard_map(
        shards,
        mesh=mesh,
        in_specs=(
            P("row", "col"), P(("col", "row"), None), P(("row", "col"), None),
            P("row", None), P("col", None),
        ),
        out_specs=(P("col", "row"), P("row", "col"), P("row"), P("col")),
        check_vma=False,
    )
```

```python
import functools

import jax
import jax.numpy as jnp
from jax import lax
from jax.experimental import pallas as pl
from jax.experimental.pallas import tpu as pltpu
from jax.sharding import PartitionSpec as P

F32 = jnp.float32
BF16 = jnp.bfloat16
MESH = pl.DeviceIdType.MESH
NODE = 512
EARLIER = 384
SAMPLES = 128
NZ = 8
ROWS = 4096
COLS = 1024
QS = 4
VMEM_LIMIT = 67043328


def three_parts(value):
    hi = value.astype(BF16).astype(F32)
    rest = value - hi
    mid = rest.astype(BF16).astype(F32)
    low = rest - mid
    return jnp.concatenate([hi, mid, low], axis=0).astype(BF16)


def joined(stacked, count):
    return stacked[:count] + stacked[count : 2 * count] + stacked[2 * count :]


def parts_dot(value, other, contract):
    out = lax.dot_general(
        three_parts(value), other, (((1,), (contract,)), ((), ())), preferred_element_type=F32
    )
    return joined(out, value.shape[0])


def kernel(
    a_hbm, r_hbm, l_hbm, rb_hbm, cb_hbm,
    row_hbm, col_hbm, rs_hbm, cs_hbm,
    row_out, col_out, rs_out, cs_out,
    a_v, rg, r_raw, l_raw, lg, rb_v, rbt, cb_v, rowacc, cacc, cr, cr4, sx, srecv, tb,
    ra_fin, rb_fin, vrow, vrow_all, vcol, vcol_all,
    in_sem, out_sem, a_sem,
    r_ss, r_rs, la_ss, la_rs, lb_ss, lb_rs, lp_ss, lp_rs,
    d_ss, d_rs, sa_ss, sa_rs, sb_ss, sb_rs, c_ss, c_rs,
    vr_ss, vr_rs, vc_ss, vc_rs,
):
    z = lax.axis_index("row")
    c = lax.axis_index("col")
    core = lax.rem(c, 2)
    other = 1 - core
    x = lax.rem(lax.div(c, 2), 4)
    y = lax.div(c, 8)
    a0 = core * y + other * x
    b0 = core * x + other * y
    stride_a = 2 + 6 * core
    stride_b = 8 - 6 * core

    def za(step):
        return lax.rem(z + step + NZ, NZ)

    def at_a(step):
        return lax.rem(a0 + step + 4, 4)

    def at_b(step):
        return lax.rem(b0 + step + 4, 4)

    def dev_a(step):
        return (z, at_a(step) * stride_a + b0 * stride_b + core)

    def dev_b(step):
        return (z, a0 * stride_a + at_b(step) * stride_b + core)

    def dev_z(step):
        return (za(step), c)

    partner = (z, c + 1 - 2 * core)

    def remote(src, dst, ssem, rsem, device):
        return pltpu.make_async_remote_copy(
            src_ref=src, dst_ref=dst, send_sem=ssem, recv_sem=rsem,
            device_id=device, device_id_type=MESH,
        )

    sent = []

    def send(copy):
        copy.start()
        sent.append(copy)

    r_in = pltpu.make_async_copy(r_hbm, r_raw, in_sem.at[0])
    l_in = pltpu.make_async_copy(l_hbm, l_raw, in_sem.at[1])
    r_in.start()
    l_in.start()
    barrier = pltpu.get_barrier_semaphore()
    peers = [dev_z(1), dev_z(-1), dev_a(1), dev_a(-1), dev_b(1), dev_b(-1), partner]
    for peer in peers:
        pl.semaphore_signal(barrier, inc=1, device_id=peer, device_id_type=MESH)
    l_in.wait()
    own_u = a0 * 4 + b0
    lg[core, own_u] = l_raw[...].T
    r_in.wait()
    rg[z] = r_raw[...].T
    rb_in = pltpu.make_async_copy(rb_hbm, rb_v, in_sem.at[2])
    cb_in = pltpu.make_async_copy(cb_hbm, cb_v, in_sem.at[3])
    rb_in.start()
    a_in = []
    for part in range(8):
        rows = pl.ds(part * NODE, NODE)
        copy = pltpu.make_async_copy(a_hbm.at[rows], a_v.at[rows], a_sem.at[part])
        copy.start()
        a_in.append(copy)
    cb_in.start()
    pl.semaphore_wait(barrier, len(peers))

    def r_copy(side, kind):
        d = 1 if side == 0 else -1
        block = za((0, -d, -d, -3 * d)[kind])
        reach = (d, d, 2 * d, d)[kind]
        ref = rg.at[block] if kind < 3 else rg.at[block, pl.ds(64 * side, 64)]
        return remote(ref, ref, r_ss.at[side, kind], r_rs.at[side, kind], dev_z(reach))

    def l_slot(ra, rb):
        return at_a(ra) * 4 + at_b(rb)

    def la_full(side):
        d = 1 if side == 0 else -1
        ref = lg.at[core, own_u]
        return remote(ref, ref, la_ss.at[0, side], la_rs.at[0, side], dev_a(d))

    def la_half(side):
        d = 1 if side == 0 else -1
        ref = lg.at[core, l_slot(-d, 0), pl.ds(64 * side, 64)]
        return remote(ref, ref, la_ss.at[1, side], la_rs.at[1, side], dev_a(d))

    def lb_full(ra, side):
        d = 1 if side == 0 else -1
        ref = lg.at[core, l_slot(ra, 0)]
        return remote(ref, ref, lb_ss.at[0, ra, side], lb_rs.at[0, ra, side], dev_b(d))

    def lb_two(ra):
        ref = lg.at[core, l_slot(ra, 0)]
        return remote(ref, ref, lb_ss.at[1, ra, 0], lb_rs.at[1, ra, 0], dev_b(2))

    def lp(ra, rb):
        ref = lg.at[core, l_slot(ra, rb)]
        return remote(ref, ref, lp_ss.at[ra, rb], lp_rs.at[ra, rb], partner)

    def lb_arrived(ra):
        for side in (0, 1):
            lb_full(ra, side).wait_recv()
            send(lp(ra, 3 if side == 0 else 1))

    def lb_two_arrived(ra):
        lb_two(ra).wait_recv()
        send(lp(ra, 2))

    def row_term(node, blocks, left):
        rows = pl.ds(pl.multiple_of(node * NODE, NODE), NODE)
        right = jnp.concatenate(
            [a_v[rows, pl.ds(pl.multiple_of(k * 128, 128), 128)] for k in blocks], axis=1
        )
        return lax.dot_general(
            left, right, (((1,), (1,)), ((), ())), preferred_element_type=F32
        )

    def row_pass(blocks, first):
        left = jnp.concatenate([rg[k] for k in blocks], axis=1)

        def body(part, carry):
            for node in (2 * part, 2 * part + 1):
                term = row_term(node, blocks, left)
                if first:
                    rowacc[node] = term
                else:
                    rowacc[node] += term
            return carry

        lax.fori_loop(0, 4, body, 0)

    def col_pass(groups, first):
        lefts, starts = [], []
        for mine, ra in groups:
            if mine:
                cc, sa, sb, a_at = core, stride_a, stride_b, at_a(ra)
            else:
                cc, sa, sb = other, 2 + 6 * other, 8 - 6 * other
                a_at = lax.rem(b0 + ra, 4)
            for b in range(4):
                lefts.append(lg[cc, a_at * 4 + b])
                starts.append(pl.multiple_of((a_at * sa + b * sb + cc) * 128, 128))
        left = jnp.concatenate(lefts, axis=1)
        right = jnp.concatenate([a_v[pl.ds(s, 128), :] for s in starts], axis=0)
        term = jnp.dot(left, right, preferred_element_type=F32).reshape(NZ, 2, 8, COLS)
        if first:
            cacc[...] = term
        else:
            cacc[...] += term

    for side in (0, 1):
        send(r_copy(side, 0))
    for side in (0, 1):
        send(la_full(side))
        send(lb_full(0, side))
    send(lp(0, 0))

    for side in (0, 1):
        r_copy(side, 0).wait_recv()
        send(r_copy(side, 1))
    for side in (0, 1):
        send(r_copy(side, 2))
    for side in (0, 1):
        la_full(side).wait_recv()
        send(la_half(side))
        ra = 3 if side == 0 else 1
        send(lb_full(ra, 0))
        send(lb_full(ra, 1))
    lb_arrived(0)
    for ra in (1, 3, 0):
        send(lb_two(ra))
    send(lp(3, 0))
    send(lp(1, 0))
    rb_in.wait()

    def turn(n, carry):
        rows = pl.ds(pl.multiple_of(n * NODE, NODE), NODE)
        rbt[n] = rb_v[rows, :].T
        return carry

    lax.fori_loop(0, 8, turn, 0)
    for copy in a_in:
        copy.wait()
    row_pass([z, za(1), za(-1)], True)

    for side in (0, 1):
        la_half(side).wait_recv()
    send(lb_full(2, 0))
    send(lb_full(2, 1))
    send(lb_two(2))
    send(lp(2, 0))
    for side in (0, 1):
        r_copy(side, 1).wait_recv()
        r_copy(side, 2).wait_recv()
        send(r_copy(side, 3))
    lb_arrived(1)
    lb_arrived(3)
    for ra in (0, 1, 3):
        lb_two_arrived(ra)
    row_pass([za(k) for k in (2, -2, 3, -3)], False)
    col_pass([(True, 0), (True, 1), (True, 3)], True)

    lb_arrived(2)
    lb_two_arrived(2)
    for side in (0, 1):
        r_copy(side, 3).wait_recv()

    last = [za(4)]
    left = jnp.concatenate([rg[k] for k in last], axis=1)
    sub = lax.broadcasted_iota(jnp.int32, (8, NODE), 0)

    def d_copy(q):
        return remote(sx.at[other, q], srecv.at[q], d_ss.at[q], d_rs.at[q], partner)

    for q in range(QS):
        for nn in (0, 1):
            total = rowacc[2 * q + nn] + row_term(2 * q + nn, last, left)
            v = total.reshape(16, 8, NODE)
            w = pltpu.roll(v, 4, 1)
            for one in range(4):
                for bp in (0, 1):
                    t0, t1 = 8 * bp + one, 8 * bp + 4 + one
                    sx[0, q, nn, one, bp] = jnp.where(sub < 4, v[t0], w[t1])
                    t0 = 4 * one + 2 * bp
                    sx[1, q, nn, one, bp] = jnp.where(sub < 4, w[t0], v[t0 + 1])
        send(d_copy(q))

    def c_copy(side, kind, n):
        d = 1 if side == 0 else -1
        lanes = pl.ds(n * NODE, NODE)
        if kind == 0:
            src, dst = cacc.at[za(4), side, :, lanes], cr4.at[side, n]
        else:
            src = cacc.at[za((0, 3 * d, d, 2 * d)[kind]), :, :, lanes]
            dst = cr.at[kind - 1, side, n]
        reach = (2 * d, d, d, 2 * d)[kind]
        return remote(
            src, dst, c_ss.at[kind, side, n], c_rs.at[kind, side, n], dev_z(reach)
        )

    def sa_copy(q, step):
        return remote(
            sx.at[core, q, :, at_a(step)], ra_fin.at[step, q],
            sa_ss.at[step, q], sa_rs.at[step, q], dev_a(step),
        )

    def sb_copy(q, step):
        return remote(
            tb.at[q, at_b(step)], rb_fin.at[step, q],
            sb_ss.at[step, q], sb_rs.at[step, q], dev_b(step),
        )

    def chip_sum(q):
        d_copy(q).wait_recv()
        full = [(sx[core, q, nn] + srecv[q, nn]).reshape(64, NODE) for nn in (0, 1)]
        coeffs = [
            parts_dot(full[nn], rb_v[pl.ds((2 * q + nn) * NODE, NODE), :], 0) for nn in (0, 1)
        ]
        cleaned = [full[nn] - parts_dot(coeffs[nn], rbt[2 * q + nn], 0) for nn in (0, 1)]
        for nn in (0, 1):
            sx[core, q, nn] = cleaned[nn].reshape(4, 2, 8, NODE)
        for step in (2, 1, 3):
            send(sa_copy(q, step))

    def a_summed(q):
        for step in (1, 3, 2):
            sa_copy(q, step).wait_recv()
        low, high = [
            sx[core, q, nn, a0] + ra_fin[1, q, nn] + ra_fin[3, q, nn] + ra_fin[2, q, nn]
            for nn in (0, 1)
        ]
        low_rolled, high_rolled = pltpu.roll(low, 4, 1), pltpu.roll(high, 4, 1)
        for bp in (0, 1):
            tb[q, 2 * bp] = jnp.where(sub < 4, low[bp], high_rolled[bp])
            tb[q, 2 * bp + 1] = jnp.where(sub < 4, low_rolled[bp], high[bp])
        for step in (1, 3, 2):
            send(sb_copy(q, step))

    chip_sum(0)

    for ra in range(4):
        for rb in range(4):
            lp(ra, rb).wait_recv()
    col_pass([(True, 2), (False, 0), (False, 1), (False, 3), (False, 2)], False)

    for n in (0, 1):
        for kind in (0, 1):
            for side in (0, 1):
                send(c_copy(side, kind, n))
    for n in (0, 1):
        for side in (0, 1):
            send(c_copy(side, 2, n))

    def c_added(n):
        lanes = pl.ds(n * NODE, NODE)
        for side in (0, 1):
            two = za(2 if side == 0 else -2)
            c_copy(side, 0, n).wait_recv()
            c_copy(side, 1, n).wait_recv()
            cacc[two, :, :, lanes] += cr[0, side, n]
            cacc[two, side, :, lanes] += cr4[side, n]
            send(c_copy(side, 3, n))

    chip_sum(1)
    chip_sum(2)
    chip_sum(3)
    a_summed(0)
    c_added(0)
    a_summed(1)
    c_added(1)
    a_summed(2)
    a_summed(3)

    lane8 = lax.broadcasted_iota(jnp.int32, (8, 128), 1)
    sub8 = lax.broadcasted_iota(jnp.int32, (8, 128), 0)
    cb_in.wait()
    col_sq = jnp.zeros((8, 128), F32)
    for n in (0, 1):
        lanes = pl.ds(n * NODE, NODE)
        for side in (0, 1):
            for kind in (2, 3):
                c_copy(side, kind, n).wait_recv()
        full = cacc[z, :, :, lanes] + cr[1, 0, n] + cr[1, 1, n] + cr[2, 0, n] + cr[2, 1, n]
        full = full.reshape(16, NODE)
        basis = cb_v[pl.ds(n * NODE, NODE), :]
        cleaned = full - parts_dot(parts_dot(full, basis, 0), basis, 1)
        col_out[:, lanes] = cleaned
        sq = jnp.sum(cleaned * cleaned, axis=1, keepdims=True)
        col_sq = col_sq + jnp.where(lane8 == n, sq[:8] + sq[8:], 0.0)
    vcol[...] = jnp.sum(col_sq, axis=0, keepdims=True)
    stores = [
        pltpu.make_async_copy(src, dst, out_sem.at[k])
        for k, (src, dst) in enumerate(
            [(row_out, row_hbm), (col_out, col_hbm), (rs_out, rs_hbm), (cs_out, cs_hbm)]
        )
    ]

    def vc_copy(j):
        return remote(vcol, vcol_all.at[j], vc_ss.at[j], vc_rs.at[j], dev_z(j))

    def vr_copy(j):
        return remote(
            vrow, vrow_all.at[j], vr_ss.at[j], vr_rs.at[j], (z, lax.rem(c + j, 32))
        )

    def loop(first, last, what):
        def body(j, carry):
            what(j)
            return carry

        lax.fori_loop(first, last, body, 0)

    loop(1, NZ, lambda j: vc_copy(j).start())
    stores[1].start()

    row_sq = jnp.zeros((8, 128), F32)
    for q in range(QS):
        for step in (1, 3, 2):
            sb_copy(q, step).wait_recv()
        cleaned = tb[q, b0] + rb_fin[1, q] + rb_fin[3, q] + rb_fin[2, q]
        row_out[:, pl.ds(2 * q * NODE, NODE)] = cleaned[:4]
        row_out[:, pl.ds((2 * q + 1) * NODE, NODE)] = cleaned[4:]
        sq = jnp.sum(cleaned * cleaned, axis=1, keepdims=True)
        place = jnp.where(sub8 < 4, 2 * q, 2 * q + 1)
        row_sq = row_sq + jnp.where(lane8 == place, sq, 0.0)
    vrow[...] = jnp.sum(row_sq, axis=0, keepdims=True)
    loop(1, 32, lambda j: vr_copy(j).start())
    stores[0].start()

    loop(1, NZ, lambda j: vc_copy(j).wait_recv())
    col_total = vcol[...]
    for j in range(1, NZ):
        col_total = col_total + vcol_all[j]
    scale = 1.0 / (SAMPLES * NODE)
    cs_out[...] = jnp.sqrt(col_total * scale)[:, :2]
    stores[3].start()

    for copy in sent:
        copy.wait_send()
    loop(1, NZ, lambda j: vc_copy(j).wait_send())

    loop(1, 32, lambda j: vr_copy(j).wait_recv())
    row_total = vrow[...]
    for j in range(1, 32):
        row_total = row_total + vrow_all[j]
    rs_out[...] = jnp.sqrt(row_total * scale)[:, :8]
    stores[2].start()
    loop(1, 32, lambda j: vr_copy(j).wait_send())
    for copy in stores:
        copy.wait()


def store_kernel(*refs):
    given, stored, held, sem = refs[:4], refs[4:8], refs[8:12], refs[12]
    loads = [pltpu.make_async_copy(given[k], held[k], sem.at[0, k]) for k in range(4)]
    stores = [pltpu.make_async_copy(held[k], stored[k], sem.at[1, k]) for k in range(4)]
    for copy in loads:
        copy.start()
    for load, store in zip(loads, stores):
        load.wait()
        store.start()
    for copy in stores:
        copy.wait()


def shards(front_matrix, right_random, left_random, row_basis, column_basis):
    vmem = pltpu.VMEM
    dma = pltpu.SemaphoreType.DMA
    row, col, rs, cs = pl.pallas_call(
        kernel,
        out_shape=(
            jax.ShapeDtypeStruct((4, ROWS), F32),
            jax.ShapeDtypeStruct((16, COLS), F32),
            jax.ShapeDtypeStruct((1, 8), F32),
            jax.ShapeDtypeStruct((1, 2), F32),
        ),
        in_specs=[pl.BlockSpec(memory_space=pltpu.HBM)] * 5,
        out_specs=[pl.BlockSpec(memory_space=pltpu.HBM)] * 4,
        scratch_shapes=[
            vmem((4, ROWS), F32), vmem((16, COLS), F32), vmem((1, 8), F32), vmem((1, 2), F32),
            vmem((ROWS, COLS), BF16),
            vmem((NZ, 128, 128), BF16),
            vmem((128, 128), BF16),
            vmem((128, 128), BF16),
            vmem((2, 16, 128, 128), BF16),
            vmem((ROWS, EARLIER), BF16),
            vmem((8, EARLIER, NODE), BF16),
            vmem((COLS, EARLIER), BF16),
            vmem((8, 128, NODE), F32),
            vmem((NZ, 2, 8, COLS), F32),
            vmem((3, 2, 2, 2, 8, NODE), F32),
            vmem((2, 2, 8, NODE), F32),
            vmem((2, QS, 2, 4, 2, 8, NODE), F32),
            vmem((QS, 2, 4, 2, 8, NODE), F32),
            vmem((QS, 4, 8, NODE), F32),
            vmem((4, QS, 2, 2, 8, NODE), F32),
            vmem((4, QS, 8, NODE), F32),
            vmem((1, 128), F32),
            vmem((32, 1, 128), F32),
            vmem((1, 128), F32),
            vmem((NZ, 1, 128), F32),
            dma((4,)), dma((4,)), dma((8,)),
            dma((2, 4)), dma((2, 4)),
            dma((2, 2)), dma((2, 2)),
            dma((2, 4, 2)), dma((2, 4, 2)),
            dma((4, 4)), dma((4, 4)),
            dma((QS,)), dma((QS,)),
            dma((4, QS)), dma((4, QS)),
            dma((4, QS)), dma((4, QS)),
            dma((4, 2, 2)), dma((4, 2, 2)),
            dma((32,)), dma((32,)),
            dma((NZ,)), dma((NZ,)),
        ],
        compiler_params=pltpu.CompilerParams(
            collective_id=0, has_side_effects=True, vmem_limit_bytes=VMEM_LIMIT
        ),
        name="hss_sample",
    )(front_matrix, right_random, left_random, row_basis, column_basis)
    results = (row, col, rs, cs)
    row, col, rs, cs = pl.pallas_call(
        store_kernel,
        out_shape=tuple(jax.ShapeDtypeStruct(v.shape, F32) for v in results),
        in_specs=[pl.BlockSpec(memory_space=pltpu.HBM)] * 4,
        out_specs=[pl.BlockSpec(memory_space=pltpu.HBM)] * 4,
        scratch_shapes=[vmem(v.shape, F32) for v in results] + [dma((2, 4))],
        compiler_params=pltpu.CompilerParams(vmem_limit_bytes=VMEM_LIMIT),
        name="store_results",
    )(*results)
    return row, col, rs.reshape(8), cs.reshape(2)


def solution(mesh):
    return jax.shard_map(
        shards,
        mesh=mesh,
        in_specs=(
            P("row", "col"), P(("col", "row"), None), P(("row", "col"), None),
            P("row", None), P("col", None),
        ),
        out_specs=(P("col", "row"), P("row", "col"), P("row"), P("col")),
        check_vma=False,
    )
```
